32 devices in a mesh: dp: 1 (over z), tp: 4 (over y), pp: 8 (over x, core).
Axes of the slice: x: 4, y: 4, z: 1, core: 2. Of those that a mesh axis runs over, the one named last changes fastest.
The devices are a block of a 4x4x8 slice.
Arguments:
- hidden_in: bfloat16 [6, 1, 768, 1536], P(None, 'dp')
- positions: int32 [6, 1, 768], P(None, 'dp')
- ln_params: float32 [8, 4, 1536], P('pp')
- w_qkv: bfloat16 [8, 1536, 3, 16, 96], P('pp', None, None, 'tp')
- b_qkv: float32 [8, 3, 16, 96], P('pp', None, 'tp')
- w_out: bfloat16 [8, 16, 96, 1536], P('pp', 'tp')
- w_up: bfloat16 [8, 1536, 6144], P('pp', None, 'tp')
- b_up: float32 [8, 6144], P('pp', 'tp')
- w_down: bfloat16 [8, 6144, 1536], P('pp', 'tp')
- b_res: float32 [8, 2, 1536], P('pp')
Outputs:
- output: bfloat16 [8, 6, 1, 768, 1536], P('pp', None, 'dp')
All inputs are finite; a program needn't handle non-finite values.
Results may differ from the reference program's by a relative error of at most 0.02.
Values are sent between devices in bfloat16 or wider.
A program may use at most 768 MiB of HBM per device.

```python
import jax
import jax.numpy as jnp
from jax import lax

NUM_STAGES = 8
NUM_MICRO = 6
MICRO_ROWS = 1
SEQ_LEN = 768
D_MODEL = 1536
NUM_HEADS = 16
HEAD_DIM = 96
FF_DIM = 6144


def setup_inputs(seed: int = 0, part: int = 0) -> dict:
    weight_keys = jax.random.split(jax.random.key(seed), 8)
    part_key = jax.random.fold_in(jax.random.key(seed + 1), part)
    data_keys = jax.random.split(part_key, 3)
    act_shape = (NUM_MICRO, MICRO_ROWS, SEQ_LEN, D_MODEL)
    hidden_in = jax.random.normal(data_keys[0], act_shape, jnp.float32).astype(jnp.bfloat16)
    steps_up = jax.random.randint(data_keys[1], (NUM_MICRO, MICRO_ROWS, SEQ_LEN), 1, 4, dtype=jnp.int32)
    starts = jax.random.randint(data_keys[2], (NUM_MICRO, MICRO_ROWS, 1), 0, SEQ_LEN, dtype=jnp.int32)
    positions = (starts + jnp.cumsum(steps_up, axis=-1)).astype(jnp.int32)
    ln_base = jnp.array([1.0, 0.0, 1.0, 0.0], jnp.float32)[None, :, None]
    ln_params = ln_base + 0.3 * jax.random.normal(weight_keys[0], (NUM_STAGES, 4, D_MODEL), jnp.float32)
    w_qkv = (jax.random.normal(weight_keys[1], (NUM_STAGES, D_MODEL, 3, NUM_HEADS, HEAD_DIM), jnp.float32) * D_MODEL ** -0.5).astype(jnp.bfloat16)
    b_qkv = 0.2 * jax.random.normal(weight_keys[2], (NUM_STAGES, 3, NUM_HEADS, HEAD_DIM), jnp.float32)
    w_out = (jax.random.normal(weight_keys[3], (NUM_STAGES, NUM_HEADS, HEAD_DIM, D_MODEL), jnp.float32) * D_MODEL ** -0.5).astype(jnp.bfloat16)
    w_up = (jax.random.normal(weight_keys[4], (NUM_STAGES, D_MODEL, FF_DIM), jnp.float32) * D_MODEL ** -0.5).astype(jnp.bfloat16)
    b_up = 0.5 * jax.random.normal(weight_keys[5], (NUM_STAGES, FF_DIM), jnp.float32)
    w_down = (jax.random.normal(weight_keys[6], (NUM_STAGES, FF_DIM, D_MODEL), jnp.float32) * FF_DIM ** -0.5).astype(jnp.bfloat16)
    b_res = 0.2 * jax.random.normal(weight_keys[7], (NUM_STAGES, 2, D_MODEL), jnp.float32)
    return dict(hidden_in=hidden_in, positions=positions, ln_params=ln_params, w_qkv=w_qkv, b_qkv=b_qkv, w_out=w_out, w_up=w_up, b_up=b_up, w_down=w_down, b_res=b_res)


def layer_norm(hidden, ln_gain, ln_shift):
    hid_f32 = hidden.astype(jnp.float32)
    row_mean = jnp.mean(hid_f32, axis=-1, keepdims=True)
    centred = hid_f32 - row_mean
    row_var = jnp.mean(centred * centred, axis=-1, keepdims=True)
    return (centred * lax.rsqrt(row_var + 1e-5) * ln_gain + ln_shift).astype(jnp.bfloat16)


def block_layer(hidden, pos_rows, layer_w):
    ln_p, w_qkv, b_qkv, w_out, w_up, b_up, w_down, b_res = layer_w
    tokens = MICRO_ROWS * SEQ_LEN
    normed = layer_norm(hidden, ln_p[0], ln_p[1])
    qkv_f = jnp.dot(normed.reshape(tokens, D_MODEL), w_qkv.reshape(D_MODEL, 3 * D_MODEL), preferred_element_type=jnp.float32)
    qkv_h = (qkv_f.reshape(MICRO_ROWS, SEQ_LEN, 3, NUM_HEADS, HEAD_DIM) + b_qkv).astype(jnp.bfloat16)
    query_h = qkv_h[:, :, 0].astype(jnp.float32)
    key_h = qkv_h[:, :, 1].astype(jnp.float32)
    value_h = qkv_h[:, :, 2].astype(jnp.float32)
    scores = jnp.einsum("bqhe,bkhe->bhqk", query_h, key_h) * HEAD_DIM ** -0.5
    head_ids = jnp.arange(NUM_HEADS, dtype=jnp.float32)
    slopes = jnp.exp2(-8.0 * (head_ids + 1.0) / NUM_HEADS)
    rel_pos = (pos_rows[:, :, None] - pos_rows[:, None, :]).astype(jnp.float32)
    scores = scores - slopes[None, :, None, None] * rel_pos[:, None, :, :]
    causal = jnp.arange(SEQ_LEN)[:, None] >= jnp.arange(SEQ_LEN)[None, :]
    scores = jnp.where(causal, scores, -1e30)
    probs_bf = jax.nn.softmax(scores, axis=-1).astype(jnp.bfloat16)
    context = jnp.einsum("bhqk,bkhe->bqhe", probs_bf.astype(jnp.float32), value_h).astype(jnp.bfloat16)
    attn_f = jnp.dot(context.reshape(tokens, D_MODEL), w_out.reshape(D_MODEL, D_MODEL), preferred_element_type=jnp.float32)
    resid_mid = (hidden.astype(jnp.float32) + attn_f.reshape(MICRO_ROWS, SEQ_LEN, D_MODEL) + b_res[0]).astype(jnp.bfloat16)
    normed_mlp = layer_norm(resid_mid, ln_p[2], ln_p[3])
    up_f = jnp.dot(normed_mlp.reshape(tokens, D_MODEL), w_up, preferred_element_type=jnp.float32) + b_up
    gelu_out = jax.nn.gelu(up_f, approximate=True).astype(jnp.bfloat16)
    down_f = jnp.dot(gelu_out, w_down, preferred_element_type=jnp.float32)
    return (resid_mid.astype(jnp.float32) + down_f.reshape(MICRO_ROWS, SEQ_LEN, D_MODEL) + b_res[1]).astype(jnp.bfloat16)


def reference(hidden_in, positions, ln_params, w_qkv, b_qkv, w_out, w_up, b_up, w_down, b_res):
    def layer_step(hidden, layer_w):
        def one_micro(micro_pair):
            return block_layer(micro_pair[0], micro_pair[1], layer_w)
        new_hidden = lax.map(one_micro, (hidden, positions))
        return new_hidden, new_hidden
    _, stage_outs = lax.scan(layer_step, hidden_in, (ln_params, w_qkv, b_qkv, w_out, w_up, b_up, w_down, b_res))
    return stage_outs
```

```python
import functools

import jax
import jax.numpy as jnp
from jax import lax
from jax.experimental import pallas as pl
from jax.experimental.pallas import tpu as pltpu
from jax.sharding import PartitionSpec as P

MESH = pl.DeviceIdType.MESH
F32 = jnp.float32
BF16 = jnp.bfloat16
CHUNKS = 2
SUBS = 2
LN_ROWS = 32
ATT_ROWS = 96
COLS = 512


class RingGather:
    def __init__(self, view, me, left, right, send, recv, base=0):
        self.view, self.me, self.left, self.right = view, me, left, right
        self.send, self.recv, self.base = send, recv, base

    def _copy(self, owner, half, slot, to):
        ref = self.view(owner, half)
        return pltpu.make_async_remote_copy(
            src_ref=ref, dst_ref=ref, send_sem=self.send.at[self.base + slot], recv_sem=self.recv.at[self.base + slot],
            device_id={"tp": to}, device_id_type=MESH)

    def start(self):
        self._copy(self.me, 0, 0, self.right).start()
        self._copy(self.me, 1, 3, self.left).start()
        self._copy(self.me, 1, 1, self.right).start()
        self._copy(self.me, 0, 4, self.left).start()

    def forward(self):
        self._copy(self.left, 0, 0, self.right).wait_recv()
        self._copy(self.left, 0, 2, self.right).start()
        self._copy(self.right, 1, 3, self.left).wait_recv()
        self._copy(self.right, 1, 5, self.left).start()

    def wait_near(self):
        self._copy(self.left, 1, 1, self.right).wait_recv()
        self._copy(self.right, 0, 4, self.left).wait_recv()

    def wait_far(self):
        far = lax.rem(self.me + 2, 4)
        self._copy(far, 0, 2, self.right).wait_recv()
        self._copy(far, 1, 5, self.left).wait_recv()

    def wait_send(self):
        for slot, owner, half, to in ((0, self.me, 0, self.right), (1, self.me, 1, self.right), (2, self.left, 0, self.right),
                                      (3, self.me, 1, self.left), (4, self.me, 0, self.left), (5, self.right, 1, self.left)):
            self._copy(owner, half, slot, to).wait_send()


def norm_rows(x, gain, shift):
    mean = jnp.mean(x, axis=-1, keepdims=True)
    cent = x - mean
    var = jnp.mean(cent * cent, axis=-1, keepdims=True)
    return (cent * lax.rsqrt(var + 1e-5) * gain + shift).astype(BF16)


def split_quarter(sub, sub_rows):
    quarter = sub_rows // 4
    big = -(-quarter // 32) * 16
    first = big if sub % 2 == 0 else quarter - big
    return (0, first), (first, quarter - first)


def pipeline_kernel(dims, slopes, hidden, pos_col, pos_row, ln_p, w_qkv, b_qkv, w_out, w_up, b_up, w_down, b_res, acts,
                    wq, wo, wu, wd, hin, a, q, kc, vc, ctx, xmid, u, part, r1, r2, msg, hout,
                    wsem, asend, arecv, rsend, rrecv, bsend, brecv, wsend, wrecv, psend, precv, osem, credit):
    n_micro, seq, width, n_local, head_dim, chunks, stages = dims
    size = seq // chunks
    sub_rows = size // SUBS
    quarter = sub_rows // 4
    local = n_local * head_dim
    units = n_micro * chunks
    ff = wu.shape[1]
    me = lax.axis_index("tp")
    stage = lax.axis_index("pp")
    left, right, far = lax.rem(me + 3, 4), lax.rem(me + 1, 4), lax.rem(me + 2, 4)
    before, after = lax.rem(stage + stages - 1, stages), lax.rem(stage + 1, stages)
    first, last = stage == 0, stage == stages - 1
    inner = jnp.logical_not(last)
    subs = range(SUBS)

    def wo_rows(owner, part_id):
        return wo.at[pl.ds(pl.multiple_of(owner * local + part_id * (local // 2), 64), local // 2)]

    own_wo = wo.at[pl.ds(pl.multiple_of(me * local, 128), local)]
    loads = [pltpu.make_async_copy(w_out, own_wo, wsem.at[0]), pltpu.make_async_copy(w_qkv, wq, wsem.at[1]),
             pltpu.make_async_copy(w_up, wu, wsem.at[2]), pltpu.make_async_copy(w_down, wd, wsem.at[3])]
    for load in loads:
        load.start()

    def fetch(unit, slot):
        m, c = unit // chunks, unit % chunks
        return pltpu.make_async_copy(hidden.at[m, pl.ds(pl.multiple_of(c * size, 64), size)], hin.at[slot], precv.at[slot])

    @pl.when(first)
    def _():
        fetch(0, 0).start()

    barrier = pltpu.get_barrier_semaphore()
    for peer in (left, right):
        pl.semaphore_signal(barrier, inc=1, device_id={"tp": peer}, device_id_type=MESH)
    for peer in (before, after):
        pl.semaphore_signal(barrier, inc=1, device_id={"pp": peer}, device_id_type=MESH)
    kc[...] = jnp.zeros_like(kc)
    vc[...] = jnp.zeros_like(vc)
    pl.semaphore_wait(barrier, 4)

    loads[0].wait()
    gather_wo = RingGather(wo_rows, me, left, right, wsend, wrecv)
    gather_wo.start()
    for load in loads[1:]:
        load.wait()

    def finish_wo():
        gather_wo.wait_near()
        gather_wo.wait_far()
        gather_wo.wait_send()

    @pl.when(jnp.logical_not(first))
    def _():
        gather_wo.forward()
        finish_wo()

    def part_rows(s, owner, k):
        offset, rows = split_quarter(s, sub_rows)[k]
        return pl.ds(pl.multiple_of(s * sub_rows + owner * quarter + offset, 16), rows)

    def quarter_rows(s, owner):
        return pl.ds(pl.multiple_of(s * sub_rows + owner * quarter, 16), quarter)

    def ctx_view(s):
        def view(owner, k):
            half = sub_rows // 2
            return ctx.at[pl.ds(s * sub_rows + k * half, half), pl.ds(pl.multiple_of(owner * local, 128), local)]
        return view

    def out_view(s):
        return lambda owner, k: hout.at[part_rows(s, owner, k)]

    gather_ctx = [RingGather(ctx_view(s), me, left, right, asend, arecv, 6 * s) for s in subs]
    gather_out = [RingGather(out_view(s), me, left, right, bsend, brecv, 6 * s) for s in subs]

    def reduce_copy(s, slot, src, dst, to):
        return pltpu.make_async_remote_copy(src_ref=src, dst_ref=dst, send_sem=rsend.at[6 * s + slot], recv_sem=rrecv.at[6 * s + slot],
                                            device_id={"tp": to}, device_id_type=MESH)

    def piece(ref, s, k):
        return ref.at[pl.ds(0, split_quarter(s, sub_rows)[k][1])]

    def copies_first(s):
        return [reduce_copy(s, 0, part.at[part_rows(s, far, 0)], piece(r1.at[s, 0], s, 0), right),
                reduce_copy(s, 1, part.at[part_rows(s, far, 1)], piece(r1.at[s, 1], s, 1), left),
                reduce_copy(s, 2, part.at[part_rows(s, right, 1)], piece(r2.at[s, 0, 1], s, 1), right),
                reduce_copy(s, 3, part.at[part_rows(s, left, 0)], piece(r2.at[s, 1, 0], s, 0), left)]

    def copies_second(s):
        return [reduce_copy(s, 4, piece(msg.at[s, 0], s, 0), piece(r2.at[s, 0, 0], s, 0), right),
                reduce_copy(s, 5, piece(msg.at[s, 1], s, 1), piece(r2.at[s, 1, 1], s, 1), left)]

    def hand_on(s, k, owner, slot):
        rows = quarter_rows(s, owner)
        return pltpu.make_async_remote_copy(src_ref=hout.at[rows], dst_ref=hin.at[slot, rows], send_sem=psend.at[4 * s + k], recv_sem=precv.at[slot],
                                            device_id={"pp": after}, device_id_type=MESH)

    def reduce_middle(s):
        firsts, seconds = copies_first(s), copies_second(s)
        for k, owner in ((0, right), (1, left)):
            rows = split_quarter(s, sub_rows)[k][1]
            firsts[k].wait_recv()
            msg[s, k, :rows, :] = (part[part_rows(s, owner, k), :].astype(F32) + r1[s, k, :rows, :].astype(F32)).astype(BF16)
            seconds[k].start()

    def reduce_end(s, unit):
        for copy in copies_first(s)[2:] + copies_second(s):
            copy.wait_recv()
        for k in range(2):
            n, rows = split_quarter(s, sub_rows)[k][1], part_rows(s, me, k)
            y = part[rows, :].astype(F32) + r2[s, 0, k, :n, :].astype(F32) + r2[s, 1, k, :n, :].astype(F32)
            hout[rows, :] = (xmid[rows, :].astype(F32) + y + b_res[1:2, :]).astype(BF16)
        gather_out[s].start()
        if s == 0:
            @pl.when(inner & (unit > 1))
            def _():
                pl.semaphore_wait(credit, 1)

        @pl.when(inner)
        def _():
            hand_on(s, 0, me, lax.rem(unit, 2)).start()
        for copy in copies_first(s) + copies_second(s):
            copy.wait_send()

    def out_near(s, unit):
        gather_out[s].wait_near()

        @pl.when(inner)
        def _():
            hand_on(s, 1, left, lax.rem(unit, 2)).start()
            hand_on(s, 2, right, lax.rem(unit, 2)).start()

    def out_far(s, unit):
        gather_out[s].wait_far()

        @pl.when(inner)
        def _():
            hand_on(s, 3, far, lax.rem(unit, 2)).start()

    def store_out(unit):
        m, c = unit // chunks, unit % chunks
        return pltpu.make_async_copy(hout, acts.at[m, pl.ds(pl.multiple_of(c * size, 64), size)], osem.at[0])

    def tail_one(unit):
        reduce_middle(SUBS - 1)
        for s in range(SUBS - 1):
            gather_out[s].forward()
            out_near(s, unit)
        reduce_end(SUBS - 1, unit)

    def tail_two(unit):
        gather_out[SUBS - 1].forward()
        for s in range(SUBS - 1):
            out_far(s, unit)

    def tail_three(unit):
        out_near(SUBS - 1, unit)
        out_far(SUBS - 1, unit)
        store_out(unit).start()

    def finish_out(unit):
        for s in subs:
            gather_out[s].wait_send()
        store_out(unit).wait()

        @pl.when(inner)
        def _():
            for s in subs:
                for k, owner in enumerate((me, left, right, far)):
                    hand_on(s, k, owner, lax.rem(unit, 2)).wait_send()

    def norm_into(src, start, count, gain, shift):
        @pl.loop(0, count // LN_ROWS)
        def _(i):
            rows = pl.ds(pl.multiple_of(start + i * LN_ROWS, LN_ROWS), LN_ROWS)
            a[rows, :] = norm_rows(src[rows, :].astype(F32), gain, shift)

    def attention(m, c_static, s):
        base = c_static * size + s * sub_rows
        reach = min(-(-(base + sub_rows) // 128) * 128, seq)
        head_of = lax.broadcasted_iota(jnp.int32, (ATT_ROWS, local), 1)
        p_row = pos_row[m][:, :reach]

        @pl.loop(0, sub_rows // ATT_ROWS)
        def _(i):
            rows = pl.ds(pl.multiple_of(s * sub_rows + i * ATT_ROWS, ATT_ROWS), ATT_ROWS)
            first_row = base + i * ATT_ROWS
            p_col = pos_col[pl.ds(pl.multiple_of(m * seq + first_row, ATT_ROWS), ATT_ROWS), :]
            rel = p_col - p_row
            keep = (lax.broadcasted_iota(jnp.int32, (ATT_ROWS, reach), 0) + first_row) >= lax.broadcasted_iota(jnp.int32, (ATT_ROWS, reach), 1)
            q_all = q[rows, :]
            total = jnp.zeros((ATT_ROWS, local), F32)
            for h in range(n_local):
                mine = (head_of >= h * head_dim) & (head_of < (h + 1) * head_dim)
                q_h = jnp.where(mine, q_all, jnp.zeros_like(q_all))
                sc = lax.dot_general(q_h, kc[:reach, :], (((1,), (1,)), ((), ())), preferred_element_type=F32)
                sc = sc * (head_dim ** -0.5) - slopes[h] * rel
                sc = jnp.where(keep, sc, -1e30)
                top = jnp.max(sc, axis=-1, keepdims=True)
                e = jnp.exp(sc - top)
                p = (e * (1.0 / jnp.sum(e, axis=-1, keepdims=True))).astype(BF16)
                o = jnp.dot(p, vc[:reach, :], preferred_element_type=F32)
                total = jnp.where(mine, o, total)
            ctx[rows, pl.ds(pl.multiple_of(me * local, 128), local)] = total.astype(BF16)

    def attend_sub(m, c, s):
        for c_static in range(chunks):
            @pl.when(c == c_static)
            def _():
                attention(m, c_static, s)

    def step(unit, carry):
        m, c = unit // chunks, unit % chunks
        slot = lax.rem(unit, 2)
        h = hin.at[slot]

        @pl.when(first)
        def _():
            @pl.when(unit + 1 < units)
            def _():
                fetch(unit + 1, lax.rem(unit + 1, 2)).start()
            fetch(unit, slot).wait()

        @pl.when(jnp.logical_not(first))
        def _():
            pltpu.make_async_remote_copy(src_ref=hout, dst_ref=h, send_sem=psend.at[0], recv_sem=precv.at[slot],
                                         device_id={"pp": before}, device_id_type=MESH).wait_recv()

        norm_into(h, 0, size, ln_p[0:1, :], ln_p[1:2, :])
        here = pl.ds(pl.multiple_of(c * size, 64), size)
        for j, (dst, rows) in enumerate(((q, pl.ds(0, size)), (kc, here), (vc, here))):
            cols = slice(j * local, (j + 1) * local)
            dst[rows, :] = (jnp.dot(a[...], wq[:, cols], preferred_element_type=F32) + b_qkv[:, cols]).astype(BF16)

        @pl.when(unit > 0)
        def _():
            tail_one(unit - 1)
        for s in subs:
            attend_sub(m, c, s)
            gather_ctx[s].start()
            if s > 0:
                gather_ctx[s - 1].forward()
            if s == 0:
                @pl.when(unit > 0)
                def _():
                    tail_two(unit - 1)
        if SUBS == 1:
            gather_ctx[0].forward()

        @pl.when(unit > 0)
        def _():
            tail_three(unit - 1)

        @pl.when(first & (unit == 0))
        def _():
            gather_wo.forward()
            finish_wo()

        for s in subs:
            rows = pl.ds(s * sub_rows, sub_rows)
            gather_ctx[s].wait_near()
            gather_ctx[s].wait_far()

            @pl.loop(0, width // COLS)
            def _(j):
                cols = pl.ds(pl.multiple_of(j * COLS, COLS), COLS)
                y = jnp.dot(ctx[rows, :], wo[:, cols], preferred_element_type=F32)
                xmid[rows, cols] = (h[rows, cols].astype(F32) + y + b_res[0:1, cols]).astype(BF16)

            if s + 1 == SUBS:
                @pl.when(jnp.logical_not(first) & (unit < units - 2))
                def _():
                    pl.semaphore_signal(credit, inc=1, device_id={"pp": before}, device_id_type=MESH)
            norm_into(xmid, s * sub_rows, sub_rows, ln_p[2:3, :], ln_p[3:4, :])
            if s == SUBS - 2:
                gather_ctx[s + 1].forward()
            if s > 0:
                if s == 1:
                    @pl.when(unit > 0)
                    def _():
                        finish_out(unit - 1)
                reduce_middle(s - 1)

            @pl.loop(0, ff // COLS)
            def _(j):
                cols = pl.ds(pl.multiple_of(j * COLS, COLS), COLS)
                y = jnp.dot(a[rows, :], wu[:, cols], preferred_element_type=F32) + b_up[:, cols]
                u[rows, cols] = jax.nn.gelu(y, approximate=True).astype(BF16)

            if s > 0:
                reduce_end(s - 1, unit)

            @pl.loop(0, width // COLS)
            def _(j):
                cols = pl.ds(pl.multiple_of(j * COLS, COLS), COLS)
                part[rows, cols] = jnp.dot(u[rows, :], wd[:, cols], preferred_element_type=F32).astype(BF16)

            for copy in copies_first(s):
                copy.start()
        for s in subs:
            gather_ctx[s].wait_send()
        return carry

    lax.fori_loop(0, units, step, 0)
    tail_one(units - 1)
    tail_two(units - 1)
    tail_three(units - 1)
    finish_out(units - 1)


def solution(mesh):
    tp_size = mesh.shape["tp"]
    stages = mesh.shape["pp"]
    assert tp_size == 4

    def stage_body(hidden_in, positions, ln_params, w_qkv, b_qkv, w_out, w_up, b_up, w_down, b_res):
        n_micro, n_rows, seq, width = hidden_in.shape
        n_micro = n_micro * n_rows
        n_local, head_dim = w_qkv.shape[3], w_qkv.shape[4]
        local = n_local * head_dim
        ff = w_up.shape[2]
        size = seq // CHUNKS
        most = split_quarter(0, size // SUBS)[0][1]
        head_ids = (lax.axis_index("tp") * n_local + jnp.arange(n_local)).astype(F32)
        slopes = jnp.exp2(-8.0 * (head_ids + 1.0) / (n_local * tp_size))
        pos = positions.reshape(n_micro, seq).astype(F32)
        dims = (n_micro, seq, width, n_local, head_dim, CHUNKS, stages)
        hbm = pl.BlockSpec(memory_space=pl.ANY)
        vmem = pl.BlockSpec(memory_space=pltpu.VMEM)
        smem = pl.BlockSpec(memory_space=pltpu.SMEM)
        dma = pltpu.SemaphoreType.DMA
        acts = pl.pallas_call(
            functools.partial(pipeline_kernel, dims),
            out_shape=jax.ShapeDtypeStruct((n_micro, seq, width), BF16),
            in_specs=[smem, hbm, vmem, vmem, vmem, hbm, vmem, hbm, hbm, vmem, hbm, vmem],
            out_specs=hbm,
            scratch_shapes=[
                pltpu.VMEM((width, 3 * local), BF16), pltpu.VMEM((tp_size * local, width), BF16),
                pltpu.VMEM((width, ff), BF16), pltpu.VMEM((ff, width), BF16),
                pltpu.VMEM((2, size, width), BF16), pltpu.VMEM((size, width), BF16),
                pltpu.VMEM((size, local), BF16), pltpu.VMEM((seq, local), BF16), pltpu.VMEM((seq, local), BF16),
                pltpu.VMEM((size, tp_size * local), BF16), pltpu.VMEM((size, width), BF16),
                pltpu.VMEM((size, ff), BF16), pltpu.VMEM((size, width), BF16),
                pltpu.VMEM((SUBS, 2, most, width), BF16), pltpu.VMEM((SUBS, 2, 2, most, width), BF16), pltpu.VMEM((SUBS, 2, most, width), BF16),
                pltpu.VMEM((size, width), BF16),
                dma((4,)), dma((6 * SUBS,)), dma((6 * SUBS,)), dma((6 * SUBS,)), dma((6 * SUBS,)), dma((6 * SUBS,)), dma((6 * SUBS,)), dma((6,)), dma((6,)),
                dma((4 * SUBS,)), dma((2,)), dma((1,)), pltpu.SemaphoreType.REGULAR,
            ],
            compiler_params=pltpu.CompilerParams(collective_id=0, has_side_effects=True, vmem_limit_bytes=60 * 1024 * 1024),
        )(slopes, hidden_in.reshape(n_micro, seq, width), pos.reshape(n_micro * seq, 1), pos.reshape(n_micro, 1, seq), ln_params[0],
          w_qkv[0].reshape(width, 3 * local), b_qkv.reshape(1, 3 * local), w_out[0].reshape(local, width), w_up[0], b_up, w_down[0], b_res[0])
        return acts.reshape((1,) + hidden_in.shape)

    in_specs = (P(None, "dp", None, None), P(None, "dp", None), P("pp", None, None), P("pp", None, None, "tp", None), P("pp", None, "tp", None), P("pp", "tp", None, None), P("pp", None, "tp"), P("pp", "tp"), P("pp", "tp", None), P("pp", None, None))
    return jax.shard_map(stage_body, mesh=mesh, in_specs=in_specs, out_specs=P("pp", None, "dp", None, None), check_vma=False)
```

```python
import functools

import jax
import jax.numpy as jnp
from jax import lax
from jax.experimental import pallas as pl
from jax.experimental.pallas import tpu as pltpu
from jax.sharding import PartitionSpec as P

MESH = pl.DeviceIdType.MESH
F32 = jnp.float32
BF16 = jnp.bfloat16
CHUNKS = 3
LN_ROWS = 32
HEAD_UNROLL = 4
COLS = 1536


class RingGather:
    def __init__(self, view, me, left, right, send, recv, base=0):
        self.view, self.me, self.left, self.right = view, me, left, right
        self.send, self.recv, self.base = send, recv, base

    def _copy(self, owner, half, slot, to):
        ref = self.view(owner, half)
        return pltpu.make_async_remote_copy(
            src_ref=ref, dst_ref=ref, send_sem=self.send.at[self.base + slot], recv_sem=self.recv.at[self.base + slot],
            device_id={"tp": to}, device_id_type=MESH)

    def start(self):
        self._copy(self.me, 0, 0, self.right).start()
        self._copy(self.me, 1, 3, self.left).start()
        self._copy(self.me, 1, 1, self.right).start()
        self._copy(self.me, 0, 4, self.left).start()

    def start_half(self, half):
        self._copy(self.me, half, half, self.right).start()
        self._copy(self.me, half, 4 - half, self.left).start()

    def forward(self):
        self._copy(self.left, 0, 0, self.right).wait_recv()
        self._copy(self.left, 0, 2, self.right).start()
        self._copy(self.right, 1, 3, self.left).wait_recv()
        self._copy(self.right, 1, 5, self.left).start()

    def wait_near(self):
        self._copy(self.left, 1, 1, self.right).wait_recv()
        self._copy(self.right, 0, 4, self.left).wait_recv()

    def wait_far(self):
        far = lax.rem(self.me + 2, 4)
        self._copy(far, 0, 2, self.right).wait_recv()
        self._copy(far, 1, 5, self.left).wait_recv()

    def wait_send(self):
        for slot, owner, half, to in ((0, self.me, 0, self.right), (1, self.me, 1, self.right), (2, self.left, 0, self.right),
                                      (3, self.me, 1, self.left), (4, self.me, 0, self.left), (5, self.right, 1, self.left)):
            self._copy(owner, half, slot, to).wait_send()


def norm_rows(x, gain, shift):
    mean = jnp.mean(x, axis=-1, keepdims=True)
    cent = x - mean
    var = jnp.mean(cent * cent, axis=-1, keepdims=True)
    return (cent * lax.rsqrt(var + 1e-5) * gain + shift).astype(BF16)


def pipeline_kernel(dims, slopes, hidden, pos_col, pos_row, ln_p, w_qkv, b_qkv, w_out, w_up, b_up, w_down, b_res, acts,
                    wq, wo, wu, wd, hin, a, qkv, ctx, xmid, u, part, r1, r2, msg, hout,
                    wsem, asend, arecv, rsend, rrecv, bsend, brecv, wsend, wrecv, psend, precv, osem, credit):
    n_micro, seq, width, n_local, head_dim, chunks, stages = dims
    size = seq // chunks
    quarter, half = size // 4, size // 8
    local = n_local * head_dim
    units = n_micro * chunks
    ff = wu.shape[1]
    me = lax.axis_index("tp")
    stage = lax.axis_index("pp")
    left, right, far = lax.rem(me + 3, 4), lax.rem(me + 1, 4), lax.rem(me + 2, 4)
    before, after = lax.rem(stage + stages - 1, stages), lax.rem(stage + 1, stages)
    first, last = stage == 0, stage == stages - 1
    inner = jnp.logical_not(last)

    def wo_rows(owner, part_id):
        return wo.at[pl.ds(pl.multiple_of(owner * local + part_id * (local // 2), 64), local // 2)]

    own_wo = wo.at[pl.ds(pl.multiple_of(me * local, 128), local)]
    loads = [pltpu.make_async_copy(w_out, own_wo, wsem.at[0]), pltpu.make_async_copy(w_qkv, wq, wsem.at[1]),
             pltpu.make_async_copy(w_up, wu, wsem.at[2]), pltpu.make_async_copy(w_down, wd, wsem.at[3])]
    for load in loads:
        load.start()

    def fetch(unit, slot):
        m, c = unit // chunks, unit % chunks
        return pltpu.make_async_copy(hidden.at[m, pl.ds(pl.multiple_of(c * size, 64), size)], hin.at[slot], precv.at[slot])

    @pl.when(first)
    def _():
        fetch(0, 0).start()

    barrier = pltpu.get_barrier_semaphore()
    for peer in (left, right):
        pl.semaphore_signal(barrier, inc=1, device_id={"tp": peer}, device_id_type=MESH)
    for peer in (before, after):
        pl.semaphore_signal(barrier, inc=1, device_id={"pp": peer}, device_id_type=MESH)
    qkv[...] = jnp.zeros_like(qkv)
    pl.semaphore_wait(barrier, 4)

    loads[0].wait()
    gather_wo = RingGather(wo_rows, me, left, right, wsend, wrecv)
    gather_wo.start()
    for load in loads[1:]:
        load.wait()

    def finish_wo():
        gather_wo.wait_near()
        gather_wo.wait_far()
        gather_wo.wait_send()

    @pl.when(jnp.logical_not(first))
    def _():
        gather_wo.forward()
        finish_wo()

    def part_rows(owner, k):
        return pl.ds(pl.multiple_of(owner * quarter + k * half, 8), half)

    def quarter_rows(owner):
        return pl.ds(pl.multiple_of(owner * quarter, 16), quarter)

    def gather_ctx(unit):
        parity = lax.rem(unit, 2)

        def view(owner, k):
            return ctx.at[parity, pl.ds(k * (size // 2), size // 2), pl.ds(pl.multiple_of(owner * local, 128), local)]
        return RingGather(view, me, left, right, asend, arecv, 6 * parity)

    def gather_out(unit):
        parity = lax.rem(unit, 2)
        return RingGather(lambda owner, k: hout.at[parity, part_rows(owner, k)], me, left, right, bsend, brecv)

    def reduce_copy(slot):
        src, dst, to = ((part.at[part_rows(far, 0)], r1.at[0], right), (part.at[part_rows(far, 1)], r1.at[1], left),
                        (part.at[part_rows(right, 1)], r2.at[0, 1], right), (part.at[part_rows(left, 0)], r2.at[1, 0], left),
                        (msg.at[0], r2.at[0, 0], right), (msg.at[1], r2.at[1, 1], left))[slot]
        return pltpu.make_async_remote_copy(src_ref=src, dst_ref=dst, send_sem=rsend.at[slot], recv_sem=rrecv.at[slot],
                                            device_id={"tp": to}, device_id_type=MESH)

    def hand_on(k, owner, unit):
        rows, slot = quarter_rows(owner), lax.rem(unit, 2)
        return pltpu.make_async_remote_copy(src_ref=hout.at[slot, rows], dst_ref=hin.at[slot, rows], send_sem=psend.at[4 * slot + k],
                                            recv_sem=precv.at[slot], device_id={"pp": after}, device_id_type=MESH)

    def reduce_middle():
        for k, owner in ((0, right), (1, left)):
            reduce_copy(k).wait_recv()
            msg[k] = (part[part_rows(owner, k), :].astype(F32) + r1[k].astype(F32)).astype(BF16)
            reduce_copy(4 + k).start()

    def reduce_end(unit):
        slot = lax.rem(unit, 2)
        for k in range(2, 6):
            reduce_copy(k).wait_recv()
        for k in range(2):
            rows = part_rows(me, k)
            y = part[rows, :].astype(F32) + r2[0, k].astype(F32) + r2[1, k].astype(F32)
            hout[slot, rows, :] = (xmid[rows, :].astype(F32) + y + b_res[1:2, :]).astype(BF16)
        gather_out(unit).start()

        @pl.when(inner & (unit > 1))
        def _():
            pl.semaphore_wait(credit, 1)

        @pl.when(inner)
        def _():
            hand_on(0, me, unit).start()
        for k in range(6):
            reduce_copy(k).wait_send()

    def out_near(unit):
        gather_out(unit).wait_near()

        @pl.when(inner)
        def _():
            hand_on(1, left, unit).start()
            hand_on(2, right, unit).start()

    def store_out(unit):
        m, c, slot = unit // chunks, unit % chunks, lax.rem(unit, 2)
        return pltpu.make_async_copy(hout.at[slot], acts.at[m, pl.ds(pl.multiple_of(c * size, 64), size)], osem.at[slot])

    def out_far(unit):
        gather_out(unit).wait_far()

        @pl.when(inner)
        def _():
            hand_on(3, far, unit).start()
        store_out(unit).start()
        gather_out(unit).wait_send()

    def finish_out(unit):
        store_out(unit).wait()

        @pl.when(inner)
        def _():
            for k, owner in enumerate((me, left, right, far)):
                hand_on(k, owner, unit).wait_send()

    def norm_into(src, start, count, gain, shift):
        @pl.loop(0, count // LN_ROWS)
        def _(i):
            rows = pl.ds(pl.multiple_of(start + i * LN_ROWS, LN_ROWS), LN_ROWS)
            a[rows, :] = norm_rows(src[rows, :].astype(F32), gain, shift)

    def attention(m, c_static, parity, gather):
        base, block = c_static * size, size // 2
        reach = min(-(-(base + size) // 128) * 128, seq)
        head_of = lax.broadcasted_iota(jnp.int32, (block, local), 1)
        p_row = pos_row[m][:, :reach]

        @pl.loop(0, 2)
        def _(i):
            first_row = base + i * block
            p_col = pos_col[pl.ds(pl.multiple_of(m * seq + first_row, 32), block), :]
            rel = p_col - p_row
            keep = (lax.broadcasted_iota(jnp.int32, (block, reach), 0) + first_row) >= lax.broadcasted_iota(jnp.int32, (block, reach), 1)
            q_all = qkv[0, pl.ds(pl.multiple_of(first_row, 32), block), :]

            def head(h, total):
                mine = (head_of >= h * head_dim) & (head_of < (h + 1) * head_dim)
                q_h = jnp.where(mine, q_all, jnp.zeros_like(q_all))
                sc = lax.dot_general(q_h, qkv[1, :reach, :], (((1,), (1,)), ((), ())), preferred_element_type=F32)
                sc = sc * (head_dim ** -0.5) - slopes[h] * rel
                sc = jnp.where(keep, sc, -1e30)
                top = jnp.max(sc, axis=-1, keepdims=True)
                e = jnp.exp(sc - top)
                p = (e * (1.0 / jnp.sum(e, axis=-1, keepdims=True))).astype(BF16)
                o = jnp.dot(p, qkv[2, :reach, :], preferred_element_type=F32)
                return jnp.where(mine, o, total)

            total = lax.fori_loop(0, n_local, head, jnp.zeros((block, local), F32), unroll=HEAD_UNROLL)
            ctx[parity, pl.ds(pl.multiple_of(i * block, 32), block), pl.ds(pl.multiple_of(me * local, 128), local)] = total.astype(BF16)
            gather.start_half(i)

    def step(unit, carry):
        m, c = unit // chunks, unit % chunks
        slot = lax.rem(unit, 2)
        h = hin.at[slot]
        ctx_now = gather_ctx(unit)

        @pl.when(first)
        def _():
            @pl.when(unit + 1 < units)
            def _():
                fetch(unit + 1, lax.rem(unit + 1, 2)).start()
            fetch(unit, slot).wait()

        @pl.when(jnp.logical_not(first))
        def _():
            pltpu.make_async_remote_copy(src_ref=hout.at[slot], dst_ref=h, send_sem=psend.at[0], recv_sem=precv.at[slot],
                                         device_id={"pp": before}, device_id_type=MESH).wait_recv()

        norm_into(h, 0, size, ln_p[0:1, :], ln_p[1:2, :])
        here = pl.ds(pl.multiple_of(c * size, 64), size)

        for j in range(3):
            cols = slice(j * local, (j + 1) * local)
            qkv[j, here, :] = (jnp.dot(a[...], wq[:, cols], preferred_element_type=F32) + b_qkv[:, cols]).astype(BF16)
        for c_static in range(chunks):
            @pl.when(c == c_static)
            def _():
                attention(m, c_static, slot, ctx_now)

        @pl.when(unit > 2)
        def _():
            finish_out(unit - 3)

        @pl.when(unit > 0)
        def _():
            reduce_middle()
        ctx_now.forward()

        @pl.when(unit > 0)
        def _():
            reduce_end(unit - 1)

        @pl.when(first & (unit == 0))
        def _():
            gather_wo.forward()
            finish_wo()
        ctx_now.wait_near()
        ctx_now.wait_far()

        @pl.loop(0, width // COLS)
        def _(j):
            cols = pl.ds(pl.multiple_of(j * COLS, COLS), COLS)
            y = jnp.dot(ctx[slot], wo[:, cols], preferred_element_type=F32)
            xmid[:, cols] = (h[:, cols].astype(F32) + y + b_res[0:1, cols]).astype(BF16)

        @pl.when(jnp.logical_not(first) & (unit < units - 2))
        def _():
            pl.semaphore_signal(credit, inc=1, device_id={"pp": before}, device_id_type=MESH)
        norm_into(xmid, 0, size, ln_p[2:3, :], ln_p[3:4, :])

        @pl.when(unit > 0)
        def _():
            gather_out(unit - 1).forward()

        @pl.loop(0, ff // COLS)
        def _(j):
            cols = pl.ds(pl.multiple_of(j * COLS, COLS), COLS)
            y = jnp.dot(a[...], wu[:, cols], preferred_element_type=F32) + b_up[:, cols]
            u[:, cols] = jax.nn.gelu(y, approximate=True).astype(BF16)

        @pl.when(unit > 0)
        def _():
            out_near(unit - 1)

        @pl.loop(0, width // COLS)
        def _(j):
            cols = pl.ds(pl.multiple_of(j * COLS, COLS), COLS)
            part[:, cols] = jnp.dot(u[...], wd[:, cols], preferred_element_type=F32).astype(BF16)

        ctx_now.wait_send()
        for k in range(4):
            reduce_copy(k).start()

        @pl.when(unit > 0)
        def _():
            out_far(unit - 1)
        return carry

    lax.fori_loop(0, units, step, 0)
    finish_out(units - 3)
    reduce_middle()
    reduce_end(units - 1)
    gather_out(units - 1).forward()
    out_near(units - 1)
    out_far(units - 1)
    finish_out(units - 2)
    finish_out(units - 1)


def solution(mesh):
    tp_size = mesh.shape["tp"]
    stages = mesh.shape["pp"]
    assert tp_size == 4

    def stage_body(hidden_in, positions, ln_params, w_qkv, b_qkv, w_out, w_up, b_up, w_down, b_res):
        n_micro, n_rows, seq, width = hidden_in.shape
        n_micro = n_micro * n_rows
        n_local, head_dim = w_qkv.shape[3], w_qkv.shape[4]
        local = n_local * head_dim
        ff = w_up.shape[2]
        size = seq // CHUNKS
        half = size // 8
        head_ids = (lax.axis_index("tp") * n_local + jnp.arange(n_local)).astype(F32)
        slopes = jnp.exp2(-8.0 * (head_ids + 1.0) / (n_local * tp_size))
        pos = positions.reshape(n_micro, seq).astype(F32)
        dims = (n_micro, seq, width, n_local, head_dim, CHUNKS, stages)
        hbm = pl.BlockSpec(memory_space=pl.ANY)
        vmem = pl.BlockSpec(memory_space=pltpu.VMEM)
        smem = pl.BlockSpec(memory_space=pltpu.SMEM)
        dma = pltpu.SemaphoreType.DMA
        acts = pl.pallas_call(
            functools.partial(pipeline_kernel, dims),
            out_shape=jax.ShapeDtypeStruct((n_micro, seq, width), BF16),
            in_specs=[smem, hbm, vmem, vmem, vmem, hbm, vmem, hbm, hbm, vmem, hbm, vmem],
            out_specs=hbm,
            scratch_shapes=[
                pltpu.VMEM((width, 3 * local), BF16), pltpu.VMEM((tp_size * local, width), BF16),
                pltpu.VMEM((width, ff), BF16), pltpu.VMEM((ff, width), BF16),
                pltpu.VMEM((2, size, width), BF16), pltpu.VMEM((size, width), BF16),
                pltpu.VMEM((3, seq, local), BF16),
                pltpu.VMEM((2, size, tp_size * local), BF16), pltpu.VMEM((size, width), BF16),
                pltpu.VMEM((size, ff), BF16), pltpu.VMEM((size, width), BF16),
                pltpu.VMEM((2, half, width), BF16), pltpu.VMEM((2, 2, half, width), BF16), pltpu.VMEM((2, half, width), BF16),
                pltpu.VMEM((2, size, width), BF16),
                dma((4,)), dma((12,)), dma((12,)), dma((6,)), dma((6,)), dma((6,)), dma((6,)), dma((6,)), dma((6,)),
                dma((8,)), dma((2,)), dma((2,)), pltpu.SemaphoreType.REGULAR,
            ],
            compiler_params=pltpu.CompilerParams(collective_id=0, has_side_effects=True, vmem_limit_bytes=60 * 1024 * 1024),
        )(slopes, hidden_in.reshape(n_micro, seq, width), pos.reshape(n_micro * seq, 1), pos.reshape(n_micro, 1, seq), ln_params[0],
          w_qkv[0].reshape(width, 3 * local), b_qkv.reshape(1, 3 * local), w_out[0].reshape(local, width), w_up[0], b_up, w_down[0], b_res[0])
        return acts.reshape((1,) + hidden_in.shape)

    in_specs = (P(None, "dp", None, None), P(None, "dp", None), P("pp", None, None), P("pp", None, None, "tp", None), P("pp", None, "tp", None), P("pp", "tp", None, None), P("pp", None, "tp"), P("pp", "tp"), P("pp", "tp", None), P("pp", None, None))
    return jax.shard_map(stage_body, mesh=mesh, in_specs=in_specs, out_specs=P("pp", None, "dp", None, None), check_vma=False)
```
